256 devices in a mesh: ep: 32 (over z, x), fsdp: 8 (over y, core).
Axes of the slice: x: 4, y: 4, z: 8, core: 2. Of those that a mesh axis runs over, the one named last changes fastest.
Arguments:
- tokens: bfloat16 [4096, 4096], P('ep', 'fsdp'), may hold values from -6 to 6
- expert_ids: int32 [4096, 2], P('ep'), may hold values from 0 to 7, all different within a row; in each aligned block of 128 rows (0 to 127, 128 to 255, ...) at most 40 rows name the same one
- gate_scores: float32 [4096, 2], P('ep'), may hold values from 0.1 to 1
- gate_weight: bfloat16 [32, 3584, 4096], P('ep', 'fsdp'), may hold values from -0.09375 to 0.09375
- up_weight: bfloat16 [32, 3584, 4096], P('ep', 'fsdp'), may hold values from -0.09375 to 0.09375
- down_weight: bfloat16 [32, 3584, 4096], P('ep', 'fsdp'), may hold values from -0.046875 to 0.046875
Outputs:
- mixed: bfloat16 [4096, 4096], P('ep', 'fsdp')
The draws below stay inside these ranges and needn't reach their ends.
Inputs may be any that keep to these rules, and one draw needn't show every extreme that they name: `expert_ids`: each row names two different experts. In each aligned block of 128 rows (the rows of one index of ep) no expert is named by more than 40 rows, a bound that some block reaches.
All inputs are finite; a program needn't handle non-finite values.
Results may differ from the reference program's by a relative error of at most 0.014.
Values may be sent and summed in bfloat16 or wider, within the bound.
No kernel may reach another device: no remote copies, remote signals or barrier semaphores. Data moves between devices by JAX's collectives and lax.ppermute only.
A program may use at most 128 MiB of HBM per device.

```python
import math
import jax
import jax.numpy as jnp
import numpy as np
from jax import lax

D = 4096
FF = 14336
EXPERTS = 8
TOK_DEV = 128
CAP = 40
TOKENS = 4096
FF_OWN = 3584
N_EP = 32
N_FSDP = 8


def block_levels(rng, extent, cuts, smallest, high):
    factor_of, own = 1.0, jax.random.fold_in(rng, 6)
    for axis_at, blocks in cuts:
        heights = jnp.exp(jax.random.uniform(jax.random.fold_in(own, axis_at), (blocks,), jnp.float32, smallest / len(cuts), high / len(cuts)))
        factor_of = factor_of * jnp.repeat(heights, extent[axis_at] // blocks).reshape([-1 if axis == axis_at else 1 for axis in range(len(extent))])
    return factor_of


def shared_out(rng, own, number, rows, amount, top, bound, slope):
    ranking = jax.random.permutation(rng, amount)
    crowded, ordinary = shares(amount, rows * top, bound, slope, True), shares(amount, rows * top, bound, slope, False)
    places = jnp.arange(amount)

    def named(tallies, rotation):
        used = int((tallies > 0).sum())
        fixed = max(1, used // 4)
        shifted = fixed + (places - fixed + rotation * (used - fixed)) % max(1, amount - fixed)
        return jnp.zeros((amount,), jnp.int32).at[ranking[jnp.where(places < fixed, places, shifted)]].set(jnp.asarray(tallies, jnp.int32))

    tallies = jnp.where(number % 4 == 0, named(crowded, number // 4), named(ordinary, number - number // 4 - 1))
    mixed = jax.random.permutation(jax.random.fold_in(own, 3), amount)
    source_of, receiver = mixed[0:amount // 2 * 2:2], mixed[1:amount // 2 * 2:2]
    slack = jnp.minimum(tallies[source_of] - 1, bound - tallies[receiver]) // 2
    slack = jnp.where((source_of == ranking[0]) | (receiver == ranking[0]) | (tallies[receiver] == 0), 0, jnp.maximum(slack, 0))
    shifted = jax.random.randint(jax.random.fold_in(own, 4), (amount // 2,), 0, 1 << 20) % (slack + 1)
    tallies = tallies.at[source_of].add(-shifted).at[receiver].add(shifted)
    items = jnp.searchsorted(jnp.cumsum(tallies), jnp.arange(rows * top), side="right").astype(jnp.int32)
    table = items.reshape(top, rows).T
    table = table[jax.random.permutation(jax.random.fold_in(own, 1), rows)]
    rotation = jax.random.randint(jax.random.fold_in(own, 2), (rows, 1), 0, top)
    return jnp.take_along_axis(table, (jnp.arange(top)[None, :] + rotation) % top, axis=1)


def shares(count, total, reach, lean, full):
    portions = [(1 << 20) // math.isqrt(grade ** lean) + 1 for grade in range(1, count + 1)]
    largest = reach if full else min(reach, max(-(-total // count), total * portions[0] // sum(portions)))
    least = 1 if total - largest >= count - 1 else 0
    holding, rest = [largest] + [least] * (count - 1), total - largest - least * (count - 1)
    while rest > 0:
        movable = [i for i in range(1, count) if holding[i] < largest] or [i for i in range(1, count) if holding[i] < reach]
        mass, left = sum([portions[i] for i in movable]), rest
        for i in movable:
            more = min(reach - holding[i], max(1, left * portions[i] // mass), rest)
            holding[i] = holding[i] + more
            rest = rest - more
    return np.array(holding)


def bell_draw(stream_key, extent, width, limit, cuts=(), held_as=jnp.bfloat16):
    array = jax.random.normal(stream_key, extent, jnp.float32) * width
    if len(cuts) > 0:
        array = block_levels(stream_key, extent, cuts, -0.22, 0.18) * array
    return jnp.clip(array, min=-limit, max=limit).astype(held_as)


def setup_inputs(seed: int = 0) -> dict:
    keys = jax.random.split(jax.random.key(seed), 7)
    tokens = bell_draw(keys[0], (TOKENS, D), 1.0, 6.0, ((0, 32), (1, 8)))
    expert_ids_keys = jax.random.split(jax.random.fold_in(keys[1], 1), TOKENS // TOK_DEV)
    expert_ids_turns = jax.random.permutation(jax.random.fold_in(keys[1], 3), TOKENS // TOK_DEV)
    expert_ids = jax.vmap(lambda own, number: shared_out(jax.random.fold_in(keys[1], 2), own, number, TOK_DEV, EXPERTS, 2, CAP, 2))(expert_ids_keys, expert_ids_turns).reshape((TOKENS, 2))
    gate_scores = jnp.clip(0.1 + 0.9 * jax.random.uniform(keys[2], (TOKENS, 2), jnp.float32) ** block_levels(keys[2], (TOKENS, 2), ((0, 32),), -0.2, 0.2), 0.1, 1.0)
    gate_weight = bell_draw(keys[3], (N_EP, FF_OWN, D), D ** -0.5, 0.09375, ((0, 32), (1, 8)))
    up_weight = bell_draw(keys[4], (N_EP, FF_OWN, D), D ** -0.5, 0.09375, ((0, 32), (1, 8)))
    down_weight = bell_draw(keys[5], (N_EP, FF_OWN, D), FF ** -0.5, 0.046875, ((0, 32), (1, 8)))
    return dict(tokens=tokens, expert_ids=expert_ids, gate_scores=gate_scores, gate_weight=gate_weight, up_weight=up_weight, down_weight=down_weight)


def reference(tokens, expert_ids, gate_scores, gate_weight, up_weight, down_weight):
    split = N_EP // EXPERTS
    groups = split * N_FSDP
    ff_dev = EXPERTS * FF // (N_EP * N_FSDP)
    labels = jnp.arange(EXPERTS, dtype=jnp.int32)
    match = expert_ids[:, :, None] == labels[None, None, :]
    chosen = jnp.sum(match.astype(jnp.int32), axis=1)
    weight_of = jnp.sum(jnp.where(match, gate_scores[:, :, None], jnp.float32(0.0)), axis=1)
    blocks = chosen.reshape(N_EP, TOK_DEV, EXPERTS)
    rank = jnp.cumsum(blocks, axis=1) - blocks
    slots = jnp.arange(CAP, dtype=jnp.int32)
    hit = (blocks[:, None, :, :] == 1) & (rank[:, None, :, :] == slots[None, :, None, None])
    local = jnp.arange(TOK_DEV, dtype=jnp.int32)
    index = jnp.sum(jnp.where(hit, local[None, None, :, None], 0), axis=2).astype(jnp.int32)
    index = index + (jnp.arange(N_EP, dtype=jnp.int32) * TOK_DEV)[:, None, None]
    index = jnp.transpose(index, (2, 0, 1)).reshape(EXPERTS, N_EP * CAP).astype(jnp.int32)
    valid = jnp.transpose(jnp.any(hit, axis=2), (2, 0, 1)).reshape(EXPERTS, N_EP * CAP)
    w_gate = gate_weight.reshape(EXPERTS, groups, ff_dev, D)
    w_up = up_weight.reshape(EXPERTS, groups, ff_dev, D)
    w_down = down_weight.reshape(EXPERTS, groups, ff_dev, D)
    columns = weight_of.T

    def one_expert(total, inputs):
        rows_index, live, gates, ups, downs, column = inputs
        rows = tokens[rows_index].astype(jnp.float32)

        def one_group(acc, weights):
            gate = jnp.dot(rows, weights[0].astype(jnp.float32).T, precision=lax.Precision.HIGHEST)
            up = jnp.dot(rows, weights[1].astype(jnp.float32).T, precision=lax.Precision.HIGHEST)
            hidden = (jax.nn.silu(gate) * up).astype(jnp.bfloat16)
            hidden = lax.optimization_barrier(hidden).astype(jnp.float32)
            part = jnp.dot(hidden, weights[2].astype(jnp.float32), precision=lax.Precision.HIGHEST).astype(jnp.bfloat16)
            part = lax.optimization_barrier(part)
            return acc + part.astype(jnp.float32), None

        start = jnp.zeros((N_EP * CAP, D), jnp.float32)
        expert_out, unused = lax.scan(one_group, start, (gates, ups, downs))
        scale = jnp.where(live, column[rows_index], jnp.float32(0.0))
        return total.at[rows_index].add(scale[:, None] * expert_out), None

    total = jnp.zeros((TOKENS, D), jnp.float32)
    total, unused = lax.scan(one_expert, total, (index, valid, w_gate, w_up, w_down, columns))
    return total.astype(jnp.bfloat16)
```

```python
import jax
import jax.numpy as jnp
from jax import lax
from jax.experimental import pallas as pl
from jax.experimental.pallas import tpu as pltpu
from jax.sharding import Mesh, PartitionSpec as P

EXPERTS = 8
CAP = 40
NX = 4
NY = 4
CHUNKS = 2


PLANE = ("x", "y", "c")


def ring(axis, shift):
    pairs = []
    for x in range(NX):
        for y in range(NY):
            for c in range(2):
                along_x = (c == 0) == (axis == 0)
                tx = (x + shift) % NX if along_x else x
                ty = y if along_x else (y + shift) % NY
                pairs.append(((x * NY + y) * 2 + c, (tx * NY + ty) * 2 + c))
    return pairs


def expert_kernel(where, g0, g1, g2, g3, wg0, wg1, wu0, wu1, wd0, wd1,
                  p0, p1, p2, p3, rows_ref, hid_ref):
    core = where[0]
    y = where[1]
    held = (g0, g1, g2, g3)
    outs = (p0, p1, p2, p3)
    n, width = g0.shape[1], g0.shape[2]

    def columns(k):
        return pl.ds(pl.multiple_of(lax.rem(y - k + NY, NY) * width, width), width)

    for flip in range(2):
        @pl.when(core == flip)
        def _():
            for r in range(4):
                for k in range(4):
                    src = held[k].at[r] if flip == 0 else held[r].at[k]
                    rows_ref[r * n:(r + 1) * n, columns(k)] = src[...]

    dims = (((1,), (1,)), ((), ()))
    for half, (wg, wu) in enumerate(((wg0, wu0), (wg1, wu1))):
        gate = lax.dot_general(rows_ref[...], wg[...], dims, preferred_element_type=jnp.float32)
        up = lax.dot_general(rows_ref[...], wu[...], dims, preferred_element_type=jnp.float32)
        hid_ref[half] = (gate / (1.0 + jnp.exp(-gate)) * up).astype(jnp.bfloat16)
    for k in range(4):
        part = jnp.dot(hid_ref[0], wd0[:, columns(k)], preferred_element_type=jnp.float32)
        part += jnp.dot(hid_ref[1], wd1[:, columns(k)], preferred_element_type=jnp.float32)
        part = part.astype(jnp.bfloat16)
        for flip in range(2):
            @pl.when(core == flip)
            def _():
                for r in range(4):
                    piece = part[r * n:(r + 1) * n]
                    if flip == 0:
                        outs[k][r] = piece
                    else:
                        outs[r][k] = piece


def expert_part(where, held, weights):
    n, width = held[0].shape[1:]
    units = weights[0].shape[0]
    vmem = pl.BlockSpec(memory_space=pltpu.VMEM)
    return pl.pallas_call(
        expert_kernel,
        out_shape=[jax.ShapeDtypeStruct(held[0].shape, jnp.bfloat16)] * 4,
        in_specs=[pl.BlockSpec(memory_space=pltpu.SMEM)] + [vmem] * 10,
        out_specs=[vmem] * 4,
        scratch_shapes=[
            pltpu.VMEM((4 * n, 4 * width), jnp.bfloat16),
            pltpu.VMEM((2, 4 * n, units), jnp.bfloat16),
        ],
        compiler_params=pltpu.CompilerParams(vmem_limit_bytes=48 * 1024 * 1024),
        cost_estimate=pl.CostEstimate(
            flops=2 * 4 * n * 4 * width * units * 6, bytes_accessed=30 << 20, transcendentals=0
        ),
    )(where, *held, *weights)


def add_up(values):
    total = values[0].astype(jnp.float32)
    for v in values[1:]:
        total = total + v.astype(jnp.float32)
    return total.astype(jnp.bfloat16)


def body(tokens, expert_ids, gate_scores, gate_weight, up_weight, down_weight):
    n_z = lax.axis_size("z")
    tok_rows, feat = tokens.shape
    half = CAP // 2
    core = lax.axis_index("c")
    where = jnp.stack([core, lax.axis_index("y")]).astype(jnp.int32)

    swap = [(0, 1), (1, 0)]
    weights = []
    for w in (gate_weight[0], up_weight[0], down_weight[0]):
        weights += [w, lax.ppermute(w, "c", swap)]

    labels = jnp.arange(EXPERTS, dtype=jnp.int32)
    match = expert_ids[:, :, None] == labels[None, None, :]
    chosen = jnp.any(match, axis=1)
    rank = jnp.cumsum(chosen.astype(jnp.int32), axis=0) - 1
    slot = jnp.sum(jnp.where(match, (rank + labels * CAP)[:, None, :], 0), axis=2)
    places = jnp.arange(EXPERTS * CAP, dtype=jnp.int32)
    take = slot[:, :, None] == places[None, None, :]
    picker = jnp.any(take, axis=1).astype(jnp.bfloat16)

    buffer = lax.dot_general(
        picker, tokens, (((0,), (0,)), ((), ())), preferred_element_type=jnp.float32
    ).astype(jnp.bfloat16)
    buffer = buffer.reshape(n_z * 2, half, feat)
    here = lax.all_to_all(buffer, ("z", "c"), split_axis=0, concat_axis=0, tiled=True)
    here = here.reshape(n_z, 2, half, feat).transpose(0, 2, 1, 3)
    here = here.reshape(CHUNKS, n_z * half // CHUNKS, 2 * feat)

    def permute(v, axis, shift):
        return lax.ppermute(v, PLANE, ring(axis, shift))

    order = (1, 3, 2)
    first = []
    for i in range(CHUNKS):
        got = {s: permute(here[i], 0, s) for s in order}
        first.append(jnp.stack([here[i], got[1], got[2], got[3]]))
    held = []
    for i in range(CHUNKS):
        got = {s: permute(first[i], 1, s) for s in order}
        held.append((first[i], got[1], got[2], got[3]))
    parts = [expert_part(where, h, weights) for h in held]
    sums = []
    for part in parts:
        got = [permute(part[s], 1, -s) for s in order]
        sums.append(add_up([part[0]] + got))
    done = []
    for total in sums:
        got = [permute(total[s], 0, -s) for s in order]
        done.append(add_up([total[0]] + got))

    back = jnp.stack(done).reshape(n_z, half, 2, feat).transpose(0, 2, 1, 3)
    back = back.reshape(n_z * 2, half, feat)
    back = lax.all_to_all(back, ("z", "c"), split_axis=0, concat_axis=0, tiled=True)
    back = back.reshape(EXPERTS * CAP, feat)
    mixed = jnp.zeros((tok_rows, feat), jnp.float32)
    for k in range(2):
        mine = jnp.dot(
            take[:, k].astype(jnp.bfloat16), back, preferred_element_type=jnp.float32
        )
        mixed = mixed + gate_scores[:, k:k + 1] * mine
    return mixed.astype(jnp.bfloat16)


def solution(mesh):
    n_ep = mesh.shape["ep"]
    fine = Mesh(mesh.devices.reshape(n_ep // NX, NX, NY, 2), ("z", "x", "y", "c"))
    ep, fsdp = ("z", "x"), ("y", "c")
    in_specs = (
        P(ep, fsdp),
        P(ep, None),
        P(ep, None),
        P(ep, fsdp, None),
        P(ep, fsdp, None),
        P(ep, fsdp, None),
    )
    return jax.shard_map(body, mesh=fine, in_specs=in_specs, out_specs=P(ep, fsdp), check_vma=False)
```

```python
import jax
import jax.numpy as jnp
from jax import lax
from jax.experimental import pallas as pl
from jax.experimental.pallas import tpu as pltpu
from jax.sharding import Mesh, PartitionSpec as P

EXPERTS = 8
CAP = 40
NX = 4
NY = 4
CHUNKS = 2
LANES = 128


PLANE = ("x", "y", "c")


def ring(axis, shift):
    pairs = []
    for x in range(NX):
        for y in range(NY):
            for c in range(2):
                along_x = (c == 0) == (axis == 0)
                tx = (x + shift) % NX if along_x else x
                ty = y if along_x else (y + shift) % NY
                pairs.append(((x * NY + y) * 2 + c, (tx * NY + ty) * 2 + c))
    return pairs


def expert_kernel(where, g0, g1, g2, g3, wg0, wg1, wu0, wu1, wd0, wd1,
                  p0, p1, p2, p3, rows_ref, hid_ref, gate_ref, held_ref, sems):
    core = where[0]
    y = where[1]
    held = (g0, g1, g2, g3)
    outs = (p0, p1, p2, p3)
    blocks = rows_ref.shape[1] // (NY * LANES)
    n, width = g0.shape[1] // blocks, blocks * LANES

    copies = [
        pltpu.make_async_copy(src, held_ref.at[i], sems.at[i])
        for i, src in enumerate((wg0, wu0, wg1, wu1, wd0, wd1))
    ]
    for copy in copies:
        copy.start()

    def columns(k):
        return pl.ds(pl.multiple_of(lax.rem(y - k + NY, NY) * width, width), width)

    def lanes(k, j):
        first = lax.rem(y - k + NY, NY) * width + j * LANES
        return pl.ds(pl.multiple_of(first, LANES), LANES)

    def store(dest, part, r):
        for j in range(blocks):
            dest[j * n:(j + 1) * n] = part[r * n:(r + 1) * n, j * LANES:(j + 1) * LANES]

    for flip in range(2):
        @pl.when(core == flip)
        def _():
            for r in range(4):
                for k in range(4):
                    src = held[k].at[r] if flip == 0 else held[r].at[k]
                    for j in range(blocks):
                        rows_ref[r * n:(r + 1) * n, lanes(k, j)] = src[j * n:(j + 1) * n]

    dims = (((1,), (1,)), ((), ()))

    @pl.loop(0, 4)
    def _(step):
        for i in range(4):
            @pl.when(step == i)
            def _():
                copies[i].wait()
        value = lax.dot_general(
            rows_ref[...], held_ref[step], dims, preferred_element_type=jnp.float32
        )

        @pl.when(lax.rem(step, 2) == 0)
        def _():
            gate_ref[...] = value

        @pl.when(lax.rem(step, 2) == 1)
        def _():
            gate = gate_ref[...]
            hid_ref[lax.div(step, 2)] = (gate / (1.0 + jnp.exp(-gate)) * value).astype(jnp.bfloat16)

    copies[4].wait()
    copies[5].wait()

    @pl.loop(0, 4)
    def _(k):
        part = jnp.dot(hid_ref[0], held_ref[4, :, columns(k)], preferred_element_type=jnp.float32)
        part += jnp.dot(hid_ref[1], held_ref[5, :, columns(k)], preferred_element_type=jnp.float32)
        part = part.astype(jnp.bfloat16)
        for i in range(4):
            @pl.when((core == 0) & (k == i))
            def _():
                for r in range(4):
                    store(outs[i].at[r], part, r)

        @pl.when(core == 1)
        def _():
            for r in range(4):
                store(outs[r].at[k], part, r)


def expert_part(where, held, weights):
    units, dim = weights[0].shape
    n = held[0].shape[1] * held[0].shape[2] * NY // dim
    vmem = pl.BlockSpec(memory_space=pltpu.VMEM)
    return pl.pallas_call(
        expert_kernel,
        out_shape=[jax.ShapeDtypeStruct(held[0].shape, jnp.bfloat16)] * 4,
        in_specs=[pl.BlockSpec(memory_space=pltpu.SMEM)] + [vmem] * 4
        + [pl.BlockSpec(memory_space=pltpu.HBM)] * 6,
        out_specs=[vmem] * 4,
        scratch_shapes=[
            pltpu.VMEM((4 * n, dim), jnp.bfloat16),
            pltpu.VMEM((2, 4 * n, units), jnp.bfloat16),
            pltpu.VMEM((4 * n, units), jnp.float32),
            pltpu.VMEM((6, units, dim), jnp.bfloat16),
            pltpu.SemaphoreType.DMA((6,)),
        ],
        compiler_params=pltpu.CompilerParams(vmem_limit_bytes=44 * 1024 * 1024),
        cost_estimate=pl.CostEstimate(
            flops=2 * 4 * n * dim * units * 6, bytes_accessed=30 << 20, transcendentals=0
        ),
    )(where, *held, *weights)


def exchange(v):
    return lax.all_to_all(v, ("z", "c"), split_axis=0, concat_axis=0, tiled=True)


def add_up(values):
    total = values[0].astype(jnp.float32)
    for v in values[1:]:
        total = total + v.astype(jnp.float32)
    return total.astype(jnp.bfloat16)


def body(tokens, expert_ids, gate_scores, gate_weight, up_weight, down_weight):
    n_z = lax.axis_size("z")
    tok_rows, feat = tokens.shape
    core = lax.axis_index("c")
    where = jnp.stack([core, lax.axis_index("y")]).astype(jnp.int32)

    swap = [(0, 1), (1, 0)]
    weights = []
    for w in (gate_weight[0], up_weight[0], down_weight[0]):
        weights += [w, lax.ppermute(w, "c", swap)]

    labels = jnp.arange(EXPERTS, dtype=jnp.int32)
    match = expert_ids[:, :, None] == labels[None, None, :]
    chosen = jnp.any(match, axis=1)
    rank = jnp.cumsum(chosen.astype(jnp.int32), axis=0) - 1
    share = CAP // CHUNKS
    n = share // 2
    blocks = feat // LANES
    chunk = lax.div(rank, share)
    left = lax.rem(rank, share)
    place = lax.div(left, n) * (n * blocks) + lax.rem(left, n)
    place = place + labels * (share * blocks)
    pick = lambda v: jnp.sum(jnp.where(match, v[:, None, :], 0), axis=2)
    chunk, place = pick(chunk), pick(place)
    size = n_z * 2 * blocks * n
    sites = jnp.arange(size, dtype=jnp.int32)
    by_block = tokens.reshape(tok_rows, blocks, LANES).transpose(1, 0, 2)
    by_block = by_block.reshape(blocks * tok_rows, LANES)

    def takes(i, k):
        spot = jnp.where(chunk[:, k] == i, place[:, k], -size)
        spot = spot[None, :] + (jnp.arange(blocks, dtype=jnp.int32) * n)[:, None]
        return spot.reshape(blocks * tok_rows)[None, :] == sites[:, None]

    z_of, rest = lax.div(sites, 2 * blocks * n), lax.rem(sites, 2 * blocks * n)
    moved = lax.div(rest, n) * (n_z * n) + z_of * n + lax.rem(rest, n)
    shuffle = (moved[None, :] == sites[:, None]).astype(jnp.bfloat16)

    def select(matrix, v, contract):
        return lax.dot_general(
            matrix, v, (((contract,), (0,)), ((), ())), preferred_element_type=jnp.float32
        )

    here = []
    for i in range(CHUNKS):
        picker = (takes(i, 0) | takes(i, 1)).astype(jnp.bfloat16)
        buffer = select(picker, by_block, 1).astype(jnp.bfloat16)
        got = exchange(buffer.reshape(n_z * 2, blocks * n, LANES)).reshape(size, LANES)
        here.append(select(shuffle, got, 1).astype(jnp.bfloat16))

    def permute(v, axis, shift):
        return lax.ppermute(v, PLANE, ring(axis, shift))

    order = (1, 3, 2)
    first = []
    for i in range(CHUNKS):
        got = {s: permute(here[i], 0, s) for s in order}
        first.append(jnp.stack([here[i], got[1], got[2], got[3]]))
    held = []
    for i in range(CHUNKS):
        got = {s: permute(first[i], 1, s) for s in order}
        held.append((first[i], got[1], got[2], got[3]))
    parts = [expert_part(where, h, weights) for h in held]
    sums = []
    for part in parts:
        got = [permute(part[s], 1, -s) for s in order]
        sums.append(add_up([part[0]] + got))
    done = []
    for total in sums:
        got = [permute(total[s], 0, -s) for s in order]
        done.append(add_up([total[0]] + got))

    mixed = jnp.zeros((blocks * tok_rows, LANES), jnp.float32)
    for i, total in enumerate(done):
        back = select(shuffle, total, 0).astype(jnp.bfloat16)
        back = exchange(back.reshape(n_z * 2, blocks * n, LANES)).reshape(size, LANES)
        for k in range(2):
            score = jnp.broadcast_to(gate_scores[:, k][None, :, None], (blocks, tok_rows, 1))
            mine = select(takes(i, k).astype(jnp.bfloat16), back, 0)
            mixed = mixed + score.reshape(blocks * tok_rows, 1) * mine
    mixed = mixed.reshape(blocks, tok_rows, LANES).transpose(1, 0, 2).reshape(tok_rows, feat)
    return mixed.astype(jnp.bfloat16)


def solution(mesh):
    n_ep = mesh.shape["ep"]
    fine = Mesh(mesh.devices.reshape(n_ep // NX, NX, NY, 2), ("z", "x", "y", "c"))
    ep, fsdp = ("z", "x"), ("y", "c")
    in_specs = (
        P(ep, fsdp),
        P(ep, None),
        P(ep, None),
        P(ep, fsdp, None),
        P(ep, fsdp, None),
        P(ep, fsdp, None),
    )
    return jax.shard_map(body, mesh=fine, in_specs=in_specs, out_specs=P(ep, fsdp), check_vma=False)
```

```python
import functools

import jax
import jax.numpy as jnp
from jax import lax
from jax.experimental import pallas as pl
from jax.experimental.pallas import tpu as pltpu
from jax.sharding import Mesh, PartitionSpec as P

EXPERTS = 8
CAP = 40
NX = 4
NY = 4
CHUNKS = 2
LANES = 128


PLANE = ("x", "y", "c")


def ring(axis, shift):
    pairs = []
    for x in range(NX):
        for y in range(NY):
            for c in range(2):
                along_x = (c == 0) == (axis == 0)
                tx = (x + shift) % NX if along_x else x
                ty = y if along_x else (y + shift) % NY
                pairs.append(((x * NY + y) * 2 + c, (tx * NY + ty) * 2 + c))
    return pairs


def expert_kernel(where, g0, g1, g2, g3, wg0, wg1, wu0, wu1, wd0, wd1,
                  p0, p1, p2, p3, rows_ref, hid_ref, gate_ref, held_ref, sems):
    core = where[0]
    y = where[1]
    held = (g0, g1, g2, g3)
    outs = (p0, p1, p2, p3)
    blocks = rows_ref.shape[1] // (NY * LANES)
    n, width = g0.shape[1] // blocks, blocks * LANES

    copies = [
        pltpu.make_async_copy(src, held_ref.at[i], sems.at[i])
        for i, src in enumerate((wg0, wu0, wg1, wu1, wd0, wd1))
    ]
    for copy in copies:
        copy.start()

    def columns(k):
        return pl.ds(pl.multiple_of(lax.rem(y - k + NY, NY) * width, width), width)

    def lanes(k, j):
        first = lax.rem(y - k + NY, NY) * width + j * LANES
        return pl.ds(pl.multiple_of(first, LANES), LANES)

    def store(dest, part, r):
        for j in range(blocks):
            dest[j * n:(j + 1) * n] = part[r * n:(r + 1) * n, j * LANES:(j + 1) * LANES]

    for flip in range(2):
        @pl.when(core == flip)
        def _():
            for r in range(4):
                for k in range(4):
                    src = held[k].at[r] if flip == 0 else held[r].at[k]
                    for j in range(blocks):
                        rows_ref[r * n:(r + 1) * n, lanes(k, j)] = src[j * n:(j + 1) * n]

    dims = (((1,), (1,)), ((), ()))

    @pl.loop(0, 4)
    def _(step):
        for i in range(4):
            @pl.when(step == i)
            def _():
                copies[i].wait()
        value = lax.dot_general(
            rows_ref[...], held_ref[step], dims, preferred_element_type=jnp.float32
        )

        @pl.when(lax.rem(step, 2) == 0)
        def _():
            gate_ref[...] = value

        @pl.when(lax.rem(step, 2) == 1)
        def _():
            gate = gate_ref[...]
            hid_ref[lax.div(step, 2)] = (gate / (1.0 + jnp.exp(-gate)) * value).astype(jnp.bfloat16)

    copies[4].wait()
    copies[5].wait()

    @pl.loop(0, 4)
    def _(k):
        part = jnp.dot(hid_ref[0], held_ref[4, :, columns(k)], preferred_element_type=jnp.float32)
        part += jnp.dot(hid_ref[1], held_ref[5, :, columns(k)], preferred_element_type=jnp.float32)
        part = part.astype(jnp.bfloat16)
        for i in range(4):
            @pl.when((core == 0) & (k == i))
            def _():
                for r in range(4):
                    store(outs[i].at[r], part, r)

        @pl.when(core == 1)
        def _():
            for r in range(4):
                store(outs[r].at[k], part, r)


def expert_part(where, held, weights):
    units, dim = weights[0].shape
    n = held[0].shape[1] * held[0].shape[2] * NY // dim
    vmem = pl.BlockSpec(memory_space=pltpu.VMEM)
    return pl.pallas_call(
        expert_kernel,
        out_shape=[jax.ShapeDtypeStruct(held[0].shape, jnp.bfloat16)] * 4,
        in_specs=[pl.BlockSpec(memory_space=pltpu.SMEM)] + [vmem] * 4
        + [pl.BlockSpec(memory_space=pltpu.HBM)] * 6,
        out_specs=[vmem] * 4,
        scratch_shapes=[
            pltpu.VMEM((4 * n, dim), jnp.bfloat16),
            pltpu.VMEM((2, 4 * n, units), jnp.bfloat16),
            pltpu.VMEM((4 * n, units), jnp.float32),
            pltpu.VMEM((6, units, dim), jnp.bfloat16),
            pltpu.SemaphoreType.DMA((6,)),
        ],
        compiler_params=pltpu.CompilerParams(vmem_limit_bytes=48 * 1024 * 1024),
        cost_estimate=pl.CostEstimate(
            flops=2 * 4 * n * dim * units * 6, bytes_accessed=30 << 20, transcendentals=0
        ),
    )(where, *held, *weights)


def dispatch_kernel(ids_ref, tokens_ref, sent_ref, spots_ref):
    tok_rows, feat = tokens_ref.shape
    blocks = feat // LANES
    share = CAP // CHUNKS
    n = share // 2
    unit = blocks * n
    expert = lax.broadcasted_iota(jnp.int32, (EXPERTS, tok_rows), 0)
    named = [ids_ref[k:k + 1] == expert for k in range(2)]
    chosen = (named[0] | named[1]).astype(jnp.float32).astype(jnp.bfloat16)
    before = lax.broadcasted_iota(jnp.int32, (tok_rows, tok_rows), 0)
    before = before < lax.broadcasted_iota(jnp.int32, (tok_rows, tok_rows), 1)
    before = before.astype(jnp.float32).astype(jnp.bfloat16)
    rank = jnp.dot(chosen, before, preferred_element_type=jnp.float32).astype(jnp.int32)
    chunk = (rank >= share).astype(jnp.int32)
    left = rank - chunk * share
    core = (left >= n).astype(jnp.int32)
    group = expert * 2 + core
    row = left - core * n
    spot = group * (CHUNKS * unit) + chunk * unit + row
    at = []
    for k in range(2):
        pick = lambda v: jnp.sum(jnp.where(named[k], v, 0), axis=0, keepdims=True)
        at.append(pick(spot))
        for i in range(CHUNKS):
            held = jnp.where(chunk == i, group * unit + row, -EXPERTS * CAP * blocks)
            spots_ref[k * CHUNKS + i:k * CHUNKS + i + 1] = pick(held)
    at = [jnp.concatenate([a + l * n for l in range(blocks)], axis=1) for a in at]
    sites = sent_ref.shape[0]
    site = lax.broadcasted_iota(jnp.int32, (sites, blocks * tok_rows), 0)
    picker = ((at[0] == site) | (at[1] == site)).astype(jnp.float32).astype(jnp.bfloat16)
    tokens = jnp.concatenate(
        [tokens_ref[:, l * LANES:(l + 1) * LANES] for l in range(blocks)], axis=0
    )
    sent_ref[...] = jnp.dot(picker, tokens, preferred_element_type=jnp.float32).astype(jnp.bfloat16)


def dispatch(ids, tokens):
    tok_rows, feat = tokens.shape
    vmem = pl.BlockSpec(memory_space=pltpu.VMEM)
    return pl.pallas_call(
        dispatch_kernel,
        out_shape=[
            jax.ShapeDtypeStruct((EXPERTS * CAP * feat // LANES, LANES), jnp.bfloat16),
            jax.ShapeDtypeStruct((2 * CHUNKS, tok_rows), jnp.int32),
        ],
        in_specs=[vmem] * 2,
        out_specs=[vmem] * 2,
        compiler_params=pltpu.CompilerParams(vmem_limit_bytes=16 * 1024 * 1024),
    )(ids, tokens)


def combine_kernel(chunk, back_ref, spots_ref, scores_ref, *refs):
    mixed_ref = refs[-1]
    tok_rows, feat = mixed_ref.shape
    n = CAP // CHUNKS // 2
    site = lax.broadcasted_iota(jnp.int32, (tok_rows, back_ref.shape[0]), 1)
    for l in range(feat // LANES):
        cols = slice(l * LANES, (l + 1) * LANES)
        total = refs[0][:, cols] if len(refs) > 1 else 0.0
        for k in range(2):
            i = k * CHUNKS + chunk
            take = spots_ref[:, i:i + 1] + l * n == site
            take = take.astype(jnp.float32).astype(jnp.bfloat16)
            mine = jnp.dot(take, back_ref[...], preferred_element_type=jnp.float32)
            total = total + scores_ref[:, k:k + 1] * mine
        mixed_ref[:, cols] = total.astype(mixed_ref.dtype)


def combine(chunk, back, spots, scores, carried, feat):
    vmem = pl.BlockSpec(memory_space=pltpu.VMEM)
    last = chunk == CHUNKS - 1
    args = (back, spots, scores) + ((carried,) if chunk else ())
    return pl.pallas_call(
        functools.partial(combine_kernel, chunk),
        out_shape=jax.ShapeDtypeStruct(
            (scores.shape[0], feat), jnp.bfloat16 if last else jnp.float32
        ),
        in_specs=[vmem] * len(args),
        out_specs=vmem,
        compiler_params=pltpu.CompilerParams(vmem_limit_bytes=16 * 1024 * 1024),
    )(*args)


def exchange(v):
    return lax.all_to_all(v, ("z", "c"), split_axis=0, concat_axis=0, tiled=True)


def add_up(values):
    total = values[0].astype(jnp.float32)
    for v in values[1:]:
        total = total + v.astype(jnp.float32)
    return total.astype(jnp.bfloat16)


def body(tokens, expert_ids, gate_scores, gate_weight, up_weight, down_weight):
    n_z = lax.axis_size("z")
    _, feat = tokens.shape
    core = lax.axis_index("c")
    where = jnp.stack([core, lax.axis_index("y")]).astype(jnp.int32)

    swap = [(0, 1), (1, 0)]
    weights = []
    for w in (gate_weight[0], up_weight[0], down_weight[0]):
        weights += [w, lax.ppermute(w, "c", swap)]

    n = CAP // CHUNKS // 2
    blocks = feat // LANES
    unit = blocks * n
    sent, spots = dispatch(expert_ids.T, tokens)
    spots = spots.T

    def select(matrix, v, contract):
        return lax.dot_general(
            matrix, v, (((contract,), (0,)), ((), ())), preferred_element_type=jnp.float32
        )

    size = n_z * 2 * unit
    sites = jnp.arange(size, dtype=jnp.int32)
    z_of, rest = lax.div(sites, 2 * unit), lax.rem(sites, 2 * unit)
    moved = lax.div(rest, n) * (n_z * n) + z_of * n + lax.rem(rest, n)
    shuffle = (moved[None, :] == sites[:, None]).astype(jnp.bfloat16)

    got = exchange(sent.reshape(n_z * 2, CHUNKS * unit, LANES))
    got = got.reshape(n_z * 2, CHUNKS, unit, LANES)
    here = jnp.stack([
        select(shuffle, got[:, i].reshape(size, LANES), 1).astype(jnp.bfloat16)
        for i in range(CHUNKS)
    ])

    def permute(v, axis, shift):
        return lax.ppermute(v, PLANE, ring(axis, shift))

    order = (1, 3, 2)
    near = {s: permute(here, 0, s) for s in order}
    held = []
    for i in range(CHUNKS):
        first = jnp.stack([here[i]] + [near[s][i] for s in (1, 2, 3)])
        far = {s: permute(first, 1, s) for s in order}
        held.append((first, far[1], far[2], far[3]))
    parts = [expert_part(where, h, weights) for h in held]

    backs = []
    for part in parts:
        got = [permute(part[s], 1, -s) for s in order]
        total = add_up([part[0]] + got)
        got = [permute(total[s], 0, -s) for s in order]
        back = select(shuffle, add_up([total[0]] + got), 0).astype(jnp.bfloat16)
        back = exchange(back.reshape(n_z * 2, unit, LANES))
        backs.append(back.reshape(size, LANES))

    mixed = None
    for i, back in enumerate(backs):
        mixed = combine(i, back, spots, gate_scores, mixed, feat)
    return mixed


def solution(mesh):
    n_ep = mesh.shape["ep"]
    fine = Mesh(mesh.devices.reshape(n_ep // NX, NX, NY, 2), ("z", "x", "y", "c"))
    ep, fsdp = ("z", "x"), ("y", "c")
    in_specs = (
        P(ep, fsdp),
        P(ep, None),
        P(ep, None),
        P(ep, fsdp, None),
        P(ep, fsdp, None),
        P(ep, fsdp, None),
    )

    return jax.shard_map(body, mesh=fine, in_specs=in_specs, out_specs=P(ep, fsdp), check_vma=False)
```

```python
import jax
import jax.numpy as jnp
from jax import lax
from jax.experimental import pallas as pl
from jax.experimental.pallas import tpu as pltpu
from jax.sharding import Mesh, PartitionSpec as P

EXPERTS = 8
CAP = 40
NX = 4
NY = 4
CHUNKS = 2
LANES = 128


PLANE = ("x", "y", "c")


def ring(axis, shift):
    pairs = []
    for x in range(NX):
        for y in range(NY):
            for c in range(2):
                along_x = (c == 0) == (axis == 0)
                tx = (x + shift) % NX if along_x else x
                ty = y if along_x else (y + shift) % NY
                pairs.append(((x * NY + y) * 2 + c, (tx * NY + ty) * 2 + c))
    return pairs


def expert_kernel(where, g0, g1, g2, g3, wg0, wg1, wu0, wu1, wd0, wd1,
                  p0, p1, p2, p3, rows_ref, hid_ref, gate_ref, held_ref, sems):
    core = where[0]
    y = where[1]
    held = (g0, g1, g2, g3)
    outs = (p0, p1, p2, p3)
    blocks = rows_ref.shape[1] // (NY * LANES)
    n, width = g0.shape[1] // blocks, blocks * LANES

    copies = [
        pltpu.make_async_copy(src, held_ref.at[i], sems.at[i])
        for i, src in enumerate((wg0, wu0, wg1, wu1, wd0, wd1))
    ]
    for copy in copies[:2]:
        copy.start()

    def columns(k):
        return pl.ds(pl.multiple_of(lax.rem(y - k + NY, NY) * width, width), width)

    def lanes(k, j):
        first = lax.rem(y - k + NY, NY) * width + j * LANES
        return pl.ds(pl.multiple_of(first, LANES), LANES)

    def store(dest, part, r):
        for j in range(blocks):
            dest[j * n:(j + 1) * n] = part[r * n:(r + 1) * n, j * LANES:(j + 1) * LANES]

    for flip in range(2):
        @pl.when(core == flip)
        def _():
            for r in range(4):
                for k in range(4):
                    src = held[k].at[r] if flip == 0 else held[r].at[k]
                    for j in range(blocks):
                        rows_ref[r * n:(r + 1) * n, lanes(k, j)] = src[j * n:(j + 1) * n]

    dims = (((1,), (1,)), ((), ()))

    @pl.loop(0, 4)
    def _(step):
        for i in range(4):
            @pl.when(step == i)
            def _():
                copies[i].wait()
                copies[i + 2].start()
        value = lax.dot_general(
            rows_ref[...], held_ref[step], dims, preferred_element_type=jnp.float32
        )

        @pl.when(lax.rem(step, 2) == 0)
        def _():
            gate_ref[...] = value

        @pl.when(lax.rem(step, 2) == 1)
        def _():
            gate = gate_ref[...]
            hid_ref[lax.div(step, 2)] = (gate / (1.0 + jnp.exp(-gate)) * value).astype(jnp.bfloat16)

    copies[4].wait()
    copies[5].wait()

    @pl.loop(0, 4)
    def _(k):
        part = jnp.dot(hid_ref[0], held_ref[4, :, columns(k)], preferred_element_type=jnp.float32)
        part += jnp.dot(hid_ref[1], held_ref[5, :, columns(k)], preferred_element_type=jnp.float32)
        part = part.astype(jnp.bfloat16)
        for i in range(4):
            @pl.when((core == 0) & (k == i))
            def _():
                for r in range(4):
                    store(outs[i].at[r], part, r)

        @pl.when(core == 1)
        def _():
            for r in range(4):
                store(outs[r].at[k], part, r)


def expert_part(where, held, weights):
    units, dim = weights[0].shape
    n = held[0].shape[1] * held[0].shape[2] * NY // dim
    vmem = pl.BlockSpec(memory_space=pltpu.VMEM)
    return pl.pallas_call(
        expert_kernel,
        out_shape=[jax.ShapeDtypeStruct(held[0].shape, jnp.bfloat16)] * 4,
        in_specs=[pl.BlockSpec(memory_space=pltpu.SMEM)] + [vmem] * 4
        + [pl.BlockSpec(memory_space=pltpu.HBM)] * 6,
        out_specs=[vmem] * 4,
        scratch_shapes=[
            pltpu.VMEM((4 * n, dim), jnp.bfloat16),
            pltpu.VMEM((2, 4 * n, units), jnp.bfloat16),
            pltpu.VMEM((4 * n, units), jnp.float32),
            pltpu.VMEM((6, units, dim), jnp.bfloat16),
            pltpu.SemaphoreType.DMA((6,)),
        ],
        compiler_params=pltpu.CompilerParams(vmem_limit_bytes=48 * 1024 * 1024),
        cost_estimate=pl.CostEstimate(
            flops=2 * 4 * n * dim * units * 6, bytes_accessed=30 << 20, transcendentals=0
        ),
    )(where, *held, *weights)


def dispatch_kernel(ids_ref, tokens_ref, sent_ref, spots_ref):
    tok_rows, feat = tokens_ref.shape
    blocks = feat // LANES
    share = CAP // CHUNKS
    n = share // 2
    unit = blocks * n
    expert = lax.broadcasted_iota(jnp.int32, (EXPERTS, tok_rows), 0)
    named = [ids_ref[k:k + 1] == expert for k in range(2)]
    chosen = (named[0] | named[1]).astype(jnp.float32).astype(jnp.bfloat16)
    before = lax.broadcasted_iota(jnp.int32, (tok_rows, tok_rows), 0)
    before = before < lax.broadcasted_iota(jnp.int32, (tok_rows, tok_rows), 1)
    before = before.astype(jnp.float32).astype(jnp.bfloat16)
    rank = jnp.dot(chosen, before, preferred_element_type=jnp.float32).astype(jnp.int32)
    chunk = (rank >= share).astype(jnp.int32)
    left = rank - chunk * share
    core = (left >= n).astype(jnp.int32)
    group = expert * 2 + core
    row = left - core * n
    spot = group * (CHUNKS * unit) + chunk * unit + row
    at = []
    for k in range(2):
        at.append(jnp.sum(jnp.where(named[k], spot, 0), axis=0, keepdims=True))
        spots_ref[k:k + 1] = at[k]
    at = [jnp.concatenate([a + l * n for l in range(blocks)], axis=1) for a in at]
    sites = sent_ref.shape[0]
    site = lax.broadcasted_iota(jnp.int32, (sites, blocks * tok_rows), 0)
    picker = ((at[0] == site) | (at[1] == site)).astype(jnp.float32).astype(jnp.bfloat16)
    tokens = jnp.concatenate(
        [tokens_ref[:, l * LANES:(l + 1) * LANES] for l in range(blocks)], axis=0
    )
    sent_ref[...] = jnp.dot(picker, tokens, preferred_element_type=jnp.float32).astype(jnp.bfloat16)


def dispatch(ids, tokens):
    tok_rows, feat = tokens.shape
    vmem = pl.BlockSpec(memory_space=pltpu.VMEM)
    return pl.pallas_call(
        dispatch_kernel,
        out_shape=[
            jax.ShapeDtypeStruct((EXPERTS * CAP * feat // LANES, LANES), jnp.bfloat16),
            jax.ShapeDtypeStruct((2, tok_rows), jnp.int32),
        ],
        in_specs=[vmem] * 2,
        out_specs=[vmem] * 2,
        compiler_params=pltpu.CompilerParams(vmem_limit_bytes=16 * 1024 * 1024),
    )(ids, tokens)


def plan_kernel(spots_ref, take_ref):
    n = CAP // CHUNKS // 2
    tok_rows = spots_ref.shape[0]
    site = lax.broadcasted_iota(jnp.int32, (tok_rows, take_ref.shape[2]), 1)
    for k in range(take_ref.shape[0]):
        for l in range(take_ref.shape[1] // tok_rows):
            take = spots_ref[:, k:k + 1] + l * n == site
            take_ref[k, l * tok_rows:(l + 1) * tok_rows] = (
                take.astype(jnp.float32).astype(jnp.bfloat16)
            )


def combine_kernel(back_ref, take_ref, scores_ref, mixed_ref):
    tok_rows = mixed_ref.shape[0]
    for l in range(mixed_ref.shape[1] // LANES):
        total = jnp.zeros((tok_rows, LANES), jnp.float32)
        for k in range(2):
            mine = jnp.dot(
                take_ref[k, l * tok_rows:(l + 1) * tok_rows], back_ref[...],
                preferred_element_type=jnp.float32,
            )
            total = total + scores_ref[:, k:k + 1] * mine
        mixed_ref[:, l * LANES:(l + 1) * LANES] = total.astype(mixed_ref.dtype)


def local_call(kernel, out, *args):
    vmem = pl.BlockSpec(memory_space=pltpu.VMEM)
    return pl.pallas_call(
        kernel,
        out_shape=out,
        in_specs=[vmem] * len(args),
        out_specs=vmem,
        compiler_params=pltpu.CompilerParams(vmem_limit_bytes=16 * 1024 * 1024),
    )(*args)


def exchange(v):
    return lax.all_to_all(v, ("z", "c"), split_axis=0, concat_axis=0, tiled=True)


def add_up(values):
    total = values[0].astype(jnp.float32)
    for v in values[1:]:
        total = total + v.astype(jnp.float32)
    return total.astype(jnp.bfloat16)


def body(tokens, expert_ids, gate_scores, gate_weight, up_weight, down_weight):
    n_z = lax.axis_size("z")
    tok_rows, feat = tokens.shape
    core = lax.axis_index("c")
    where = jnp.stack([core, lax.axis_index("y")]).astype(jnp.int32)

    swap = [(0, 1), (1, 0)]
    weights = []
    for w in (gate_weight[0], up_weight[0], down_weight[0]):
        weights += [w, lax.ppermute(w, "c", swap)]

    n = CAP // CHUNKS // 2
    blocks = feat // LANES
    unit = blocks * n
    sent, spots = dispatch(expert_ids.T, tokens)
    spots = spots.T

    def select(matrix, v, contract):
        return lax.dot_general(
            matrix, v, (((contract,), (0,)), ((), ())), preferred_element_type=jnp.float32
        )

    size = n_z * 2 * unit
    sites = jnp.arange(size, dtype=jnp.int32)
    z_of, rest = lax.div(sites, 2 * unit), lax.rem(sites, 2 * unit)
    moved = lax.div(rest, n) * (n_z * n) + z_of * n + lax.rem(rest, n)
    shuffle = (moved[None, :] == sites[:, None]).astype(jnp.bfloat16)

    got = exchange(sent.reshape(n_z * 2, CHUNKS * unit, LANES))
    got = got.reshape(n_z * 2, CHUNKS, unit, LANES)
    here = jnp.stack([
        select(shuffle, got[:, i].reshape(size, LANES), 1).astype(jnp.bfloat16)
        for i in range(CHUNKS)
    ])

    def permute(v, axis, shift):
        return lax.ppermute(v, PLANE, ring(axis, shift))

    order = (1, 3, 2)
    near = {s: permute(here, 0, s) for s in order}
    held = []
    for i in range(CHUNKS):
        first = jnp.stack([here[i]] + [near[s][i] for s in (1, 2, 3)])
        far = {s: permute(first, 1, s) for s in order}
        held.append((first, far[1], far[2], far[3]))
    parts = [expert_part(where, h, weights) for h in held]

    backs = []
    for part in parts:
        got = [permute(part[s], 1, -s) for s in order]
        total = add_up([part[0]] + got)
        got = [permute(total[s], 0, -s) for s in order]
        back = select(shuffle, add_up([total[0]] + got), 0).astype(jnp.bfloat16)
        backs.append(back.reshape(n_z * 2, unit, LANES))

    back = exchange(jnp.concatenate(backs, axis=1)).reshape(CHUNKS * size, LANES)
    tok_rows = tokens.shape[0]
    take = local_call(
        plan_kernel,
        jax.ShapeDtypeStruct((2, blocks * tok_rows, CHUNKS * size), jnp.bfloat16),
        spots,
    )
    return local_call(
        combine_kernel, jax.ShapeDtypeStruct(tokens.shape, tokens.dtype), back, take, gate_scores
    )


def solution(mesh):
    n_ep = mesh.shape["ep"]
    fine = Mesh(mesh.devices.reshape(n_ep // NX, NX, NY, 2), ("z", "x", "y", "c"))
    ep, fsdp = ("z", "x"), ("y", "c")
    in_specs = (
        P(ep, fsdp),
        P(ep, None),
        P(ep, None),
        P(ep, fsdp, None),
        P(ep, fsdp, None),
        P(ep, fsdp, None),
    )

    return jax.shard_map(body, mesh=fine, in_specs=in_specs, out_specs=P(ep, fsdp), check_vma=False)
```

```python
import jax
import jax.numpy as jnp
from jax import lax
from jax.experimental import pallas as pl
from jax.experimental.pallas import tpu as pltpu
from jax.sharding import Mesh, PartitionSpec as P

EXPERTS = 8
CAP = 40
NX = 4
NY = 4
CHUNKS = 2
LANES = 128


PLANE = ("x", "y", "c")


def ring(axis, shift):
    pairs = []
    for x in range(NX):
        for y in range(NY):
            for c in range(2):
                along_x = (c == 0) == (axis == 0)
                tx = (x + shift) % NX if along_x else x
                ty = y if along_x else (y + shift) % NY
                pairs.append(((x * NY + y) * 2 + c, (tx * NY + ty) * 2 + c))
    return pairs


def expert_kernel(where, g0, g1, g2, g3, wg0, wg1, wu0, wu1, wd0, wd1,
                  p0, p1, p2, p3, rows_ref, hid_ref, gate_ref, held_ref, down_ref, sems):
    core = where[0]
    y = where[1]
    held = (g0, g1, g2, g3)
    outs = (p0, p1, p2, p3)
    blocks = rows_ref.shape[1] // (NY * LANES)
    n, width = g0.shape[1] // blocks, blocks * LANES

    units = wd0.shape[0]
    targets = [held_ref.at[i] for i in range(4)]
    targets += [down_ref.at[pl.ds(i * units, units)] for i in range(2)]
    copies = [
        pltpu.make_async_copy(src, dst, sems.at[i])
        for i, (src, dst) in enumerate(zip((wg0, wu0, wg1, wu1, wd0, wd1), targets))
    ]
    for copy in copies:
        copy.start()

    def columns(k):
        return pl.ds(pl.multiple_of(lax.rem(y - k + NY, NY) * width, width), width)

    def lanes(k, j):
        first = lax.rem(y - k + NY, NY) * width + j * LANES
        return pl.ds(pl.multiple_of(first, LANES), LANES)

    def store(dest, part, r):
        for j in range(blocks):
            dest[j * n:(j + 1) * n] = part[r * n:(r + 1) * n, j * LANES:(j + 1) * LANES]

    for flip in range(2):
        @pl.when(core == flip)
        def _():
            for r in range(4):
                for k in range(4):
                    src = held[k].at[r] if flip == 0 else held[r].at[k]
                    for j in range(blocks):
                        rows_ref[r * n:(r + 1) * n, lanes(k, j)] = src[j * n:(j + 1) * n]

    dims = (((1,), (1,)), ((), ()))

    @pl.loop(0, 4)
    def _(step):
        for i in range(4):
            @pl.when(step == i)
            def _():
                copies[i].wait()
        value = lax.dot_general(
            rows_ref[...], held_ref[step], dims, preferred_element_type=jnp.float32
        )

        @pl.when(lax.rem(step, 2) == 0)
        def _():
            gate_ref[...] = value

        @pl.when(lax.rem(step, 2) == 1)
        def _():
            gate = gate_ref[...]
            hidden = (gate / (1.0 + jnp.exp(-gate)) * value).astype(jnp.bfloat16)
            for i in range(2):
                @pl.when(step == 2 * i + 1)
                def _():
                    hid_ref[:, i * units:(i + 1) * units] = hidden

    copies[4].wait()
    copies[5].wait()

    @pl.loop(0, 4)
    def _(k):
        part = jnp.dot(hid_ref[...], down_ref[:, columns(k)], preferred_element_type=jnp.float32)
        part = part.astype(jnp.bfloat16)
        for i in range(4):
            @pl.when((core == 0) & (k == i))
            def _():
                for r in range(4):
                    store(outs[i].at[r], part, r)

        @pl.when(core == 1)
        def _():
            for r in range(4):
                store(outs[r].at[k], part, r)


def expert_part(where, held, weights):
    units, dim = weights[0].shape
    n = held[0].shape[1] * held[0].shape[2] * NY // dim
    vmem = pl.BlockSpec(memory_space=pltpu.VMEM)
    return pl.pallas_call(
        expert_kernel,
        out_shape=[jax.ShapeDtypeStruct(held[0].shape, jnp.bfloat16)] * 4,
        in_specs=[pl.BlockSpec(memory_space=pltpu.SMEM)] + [vmem] * 4
        + [pl.BlockSpec(memory_space=pltpu.HBM)] * 6,
        out_specs=[vmem] * 4,
        scratch_shapes=[
            pltpu.VMEM((4 * n, dim), jnp.bfloat16),
            pltpu.VMEM((4 * n, 2 * units), jnp.bfloat16),
            pltpu.VMEM((4 * n, units), jnp.float32),
            pltpu.VMEM((4, units, dim), jnp.bfloat16),
            pltpu.VMEM((2 * units, dim), jnp.bfloat16),
            pltpu.SemaphoreType.DMA((6,)),
        ],
        compiler_params=pltpu.CompilerParams(vmem_limit_bytes=48 * 1024 * 1024),
        cost_estimate=pl.CostEstimate(
            flops=2 * 4 * n * dim * units * 6, bytes_accessed=30 << 20, transcendentals=0
        ),
    )(where, *held, *weights)


def dispatch_kernel(ids_hbm, tokens_hbm, sent_ref, spots_ref, ids_ref, tokens_ref, sems):
    ids_copy = pltpu.make_async_copy(ids_hbm, ids_ref, sems.at[0])
    tokens_copy = pltpu.make_async_copy(tokens_hbm, tokens_ref, sems.at[1])
    ids_copy.start()
    tokens_copy.start()
    tok_rows, feat = tokens_ref.shape
    blocks = feat // LANES
    share = CAP // CHUNKS
    n = share // 2
    unit = blocks * n
    expert = lax.broadcasted_iota(jnp.int32, (EXPERTS, tok_rows), 0)
    ids_copy.wait()
    named = [ids_ref[k:k + 1] == expert for k in range(2)]
    chosen = (named[0] | named[1]).astype(jnp.float32).astype(jnp.bfloat16)
    before = lax.broadcasted_iota(jnp.int32, (tok_rows, tok_rows), 0)
    before = before < lax.broadcasted_iota(jnp.int32, (tok_rows, tok_rows), 1)
    before = before.astype(jnp.float32).astype(jnp.bfloat16)
    rank = jnp.dot(chosen, before, preferred_element_type=jnp.float32).astype(jnp.int32)
    chunk = (rank >= share).astype(jnp.int32)
    left = rank - chunk * share
    core = (left >= n).astype(jnp.int32)
    group = expert * 2 + core
    row = left - core * n
    spot = group * (CHUNKS * unit) + chunk * unit + row
    at = []
    for k in range(2):
        at.append(jnp.sum(jnp.where(named[k], spot, 0), axis=0, keepdims=True))
        spots_ref[k:k + 1] = at[k]
    at = [jnp.concatenate([a + l * n for l in range(blocks)], axis=1) for a in at]
    sites = sent_ref.shape[0]
    site = lax.broadcasted_iota(jnp.int32, (sites, blocks * tok_rows), 0)
    picker = ((at[0] == site) | (at[1] == site)).astype(jnp.float32).astype(jnp.bfloat16)
    tokens_copy.wait()
    tokens = jnp.concatenate(
        [tokens_ref[:, l * LANES:(l + 1) * LANES] for l in range(blocks)], axis=0
    )
    sent_ref[...] = jnp.dot(picker, tokens, preferred_element_type=jnp.float32).astype(jnp.bfloat16)


def dispatch(ids, tokens):
    tok_rows, feat = tokens.shape
    vmem = pl.BlockSpec(memory_space=pltpu.VMEM)
    return pl.pallas_call(
        dispatch_kernel,
        out_shape=[
            jax.ShapeDtypeStruct((EXPERTS * CAP * feat // LANES, LANES), jnp.bfloat16),
            jax.ShapeDtypeStruct((2, tok_rows), jnp.int32),
        ],
        in_specs=[pl.BlockSpec(memory_space=pltpu.HBM)] * 2,
        out_specs=[vmem] * 2,
        scratch_shapes=[
            pltpu.VMEM(ids.shape, ids.dtype),
            pltpu.VMEM(tokens.shape, tokens.dtype),
            pltpu.SemaphoreType.DMA((2,)),
        ],
        compiler_params=pltpu.CompilerParams(vmem_limit_bytes=64 * 1024 * 1024 - 65536),
    )(ids, tokens)


def plan_kernel(spots_ref, take_ref):
    n = CAP // CHUNKS // 2
    tok_rows = spots_ref.shape[0]
    site = lax.broadcasted_iota(jnp.int32, (tok_rows, take_ref.shape[2]), 1)
    for k in range(2):
        for l in range(take_ref.shape[0]):
            take = spots_ref[:, k:k + 1] + l * n == site
            take_ref[l, k * tok_rows:(k + 1) * tok_rows] = (
                take.astype(jnp.float32).astype(jnp.bfloat16)
            )


def combine_kernel(back_ref, take_ref, scores_ref, mixed_ref):
    tok_rows = mixed_ref.shape[0]
    for l in range(mixed_ref.shape[1] // LANES):
        mine = jnp.dot(take_ref[l], back_ref[...], preferred_element_type=jnp.float32)
        total = scores_ref[:, :1] * mine[:tok_rows] + scores_ref[:, 1:] * mine[tok_rows:]
        mixed_ref[:, l * LANES:(l + 1) * LANES] = total.astype(mixed_ref.dtype)


def local_call(kernel, out, *args):
    vmem = pl.BlockSpec(memory_space=pltpu.VMEM)
    return pl.pallas_call(
        kernel,
        out_shape=out,
        in_specs=[vmem] * len(args),
        out_specs=vmem,
        compiler_params=pltpu.CompilerParams(vmem_limit_bytes=16 * 1024 * 1024),
    )(*args)


def exchange(v):
    return lax.all_to_all(v, ("z", "c"), split_axis=0, concat_axis=0, tiled=True)


def add_up(values):
    total = values[0].astype(jnp.float32)
    for v in values[1:]:
        total = total + v.astype(jnp.float32)
    return total.astype(jnp.bfloat16)


def body(tokens, expert_ids, gate_scores, gate_weight, up_weight, down_weight):
    n_z = lax.axis_size("z")
    tok_rows, feat = tokens.shape
    core = lax.axis_index("c")
    where = jnp.stack([core, lax.axis_index("y")]).astype(jnp.int32)

    swap = [(0, 1), (1, 0)]
    weights = []
    for w in (gate_weight[0], up_weight[0], down_weight[0]):
        weights += [w, lax.ppermute(w, "c", swap)]

    n = CAP // CHUNKS // 2
    blocks = feat // LANES
    unit = blocks * n
    sent, spots = dispatch(expert_ids.T, tokens)
    spots = spots.T

    def select(matrix, v, contract):
        return lax.dot_general(
            matrix, v, (((contract,), (0,)), ((), ())), preferred_element_type=jnp.float32
        )

    size = n_z * 2 * unit
    sites = jnp.arange(size, dtype=jnp.int32)
    z_of, rest = lax.div(sites, 2 * unit), lax.rem(sites, 2 * unit)
    moved = lax.div(rest, n) * (n_z * n) + z_of * n + lax.rem(rest, n)
    shuffle = (moved[None, :] == sites[:, None]).astype(jnp.bfloat16)

    got = exchange(sent.reshape(n_z * 2, CHUNKS * unit, LANES))
    got = got.reshape(n_z * 2, CHUNKS, unit, LANES)
    here = jnp.stack([
        select(shuffle, got[:, i].reshape(size, LANES), 1).astype(jnp.bfloat16)
        for i in range(CHUNKS)
    ])

    def permute(v, axis, shift):
        return lax.ppermute(v, PLANE, ring(axis, shift))

    order = (1, 3, 2)
    near = {s: permute(here, 0, s) for s in order}
    held = []
    for i in range(CHUNKS):
        first = jnp.stack([here[i]] + [near[s][i] for s in (1, 2, 3)])
        far = {s: permute(first, 1, s) for s in order}
        held.append((first, far[1], far[2], far[3]))
    parts = [expert_part(where, h, weights) for h in held]

    backs = []
    for part in parts:
        got = [permute(part[s], 1, -s) for s in order]
        total = add_up([part[0]] + got)
        got = [permute(total[s], 0, -s) for s in order]
        back = select(shuffle, add_up([total[0]] + got), 0).astype(jnp.bfloat16)
        backs.append(back.reshape(n_z * 2, unit, LANES))

    back = exchange(jnp.concatenate(backs, axis=1)).reshape(CHUNKS * size, LANES)
    tok_rows = tokens.shape[0]
    take = local_call(
        plan_kernel,
        jax.ShapeDtypeStruct((blocks, 2 * tok_rows, CHUNKS * size), jnp.bfloat16),
        spots,
    )
    return local_call(
        combine_kernel, jax.ShapeDtypeStruct(tokens.shape, tokens.dtype), back, take, gate_scores
    )


def solution(mesh):
    n_ep = mesh.shape["ep"]
    fine = Mesh(mesh.devices.reshape(n_ep // NX, NX, NY, 2), ("z", "x", "y", "c"))
    ep, fsdp = ("z", "x"), ("y", "c")
    in_specs = (
        P(ep, fsdp),
        P(ep, None),
        P(ep, None),
        P(ep, fsdp, None),
        P(ep, fsdp, None),
        P(ep, fsdp, None),
    )

    return jax.shard_map(body, mesh=fine, in_specs=in_specs, out_specs=P(ep, fsdp), check_vma=False)
```

```python
import jax
import jax.numpy as jnp
from jax import lax
from jax.experimental import pallas as pl
from jax.experimental.pallas import tpu as pltpu
from jax.sharding import Mesh, PartitionSpec as P

EXPERTS = 8
CAP = 40
NX = 4
NY = 4
CHUNKS = 2
LANES = 128


PLANE = ("x", "y", "c")


def ring(axis, shift):
    pairs = []
    for x in range(NX):
        for y in range(NY):
            for c in range(2):
                along_x = (c == 0) == (axis == 0)
                tx = (x + shift) % NX if along_x else x
                ty = y if along_x else (y + shift) % NY
                pairs.append(((x * NY + y) * 2 + c, (tx * NY + ty) * 2 + c))
    return pairs


def expert_kernel(where, g0, g1, g2, g3, wg0, wg1, wu0, wu1, wd0, wd1,
                  p0, p1, p2, p3, rows_ref, hid_ref, gate_ref, held_ref, sems):
    core = where[0]
    y = where[1]
    held = (g0, g1, g2, g3)
    outs = (p0, p1, p2, p3)
    blocks = rows_ref.shape[1] // (NY * LANES)
    n, width = g0.shape[1] // blocks, blocks * LANES

    copies = [
        pltpu.make_async_copy(src, held_ref.at[i], sems.at[i])
        for i, src in enumerate((wg0, wu0, wg1, wu1, wd0, wd1))
    ]
    for copy in copies:
        copy.start()

    def columns(k):
        return pl.ds(pl.multiple_of(lax.rem(y - k + NY, NY) * width, width), width)

    def lanes(k, j):
        first = lax.rem(y - k + NY, NY) * width + j * LANES
        return pl.ds(pl.multiple_of(first, LANES), LANES)

    def store(dest, part, r):
        for j in range(blocks):
            dest[j * n:(j + 1) * n] = part[r * n:(r + 1) * n, j * LANES:(j + 1) * LANES]

    for flip in range(2):
        @pl.when(core == flip)
        def _():
            for r in range(4):
                for k in range(4):
                    src = held[k].at[r] if flip == 0 else held[r].at[k]
                    for j in range(blocks):
                        rows_ref[r * n:(r + 1) * n, lanes(k, j)] = src[j * n:(j + 1) * n]

    dims = (((1,), (1,)), ((), ()))

    @pl.loop(0, 4)
    def _(step):
        for i in range(4):
            @pl.when(step == i)
            def _():
                copies[i].wait()
        value = lax.dot_general(
            rows_ref[...], held_ref[step], dims, preferred_element_type=jnp.float32
        )

        @pl.when(lax.rem(step, 2) == 0)
        def _():
            gate_ref[...] = value

        @pl.when(lax.rem(step, 2) == 1)
        def _():
            gate = gate_ref[...]
            hid_ref[lax.div(step, 2)] = (gate / (1.0 + jnp.exp(-gate)) * value).astype(jnp.bfloat16)

    copies[4].wait()
    copies[5].wait()

    @pl.loop(0, 4)
    def _(k):
        part = jnp.dot(hid_ref[0], held_ref[4, :, columns(k)], preferred_element_type=jnp.float32)
        part += jnp.dot(hid_ref[1], held_ref[5, :, columns(k)], preferred_element_type=jnp.float32)
        part = part.astype(jnp.bfloat16)
        for i in range(4):
            @pl.when((core == 0) & (k == i))
            def _():
                for r in range(4):
                    store(outs[i].at[r], part, r)

        @pl.when(core == 1)
        def _():
            for r in range(4):
                store(outs[r].at[k], part, r)


def expert_part(where, held, weights):
    units, dim = weights[0].shape
    n = held[0].shape[1] * held[0].shape[2] * NY // dim
    vmem = pl.BlockSpec(memory_space=pltpu.VMEM)
    return pl.pallas_call(
        expert_kernel,
        out_shape=[jax.ShapeDtypeStruct(held[0].shape, jnp.bfloat16)] * 4,
        in_specs=[pl.BlockSpec(memory_space=pltpu.SMEM)] + [vmem] * 5
        + [pl.BlockSpec(memory_space=pltpu.HBM)] * 5,
        out_specs=[vmem] * 4,
        scratch_shapes=[
            pltpu.VMEM((4 * n, dim), jnp.bfloat16),
            pltpu.VMEM((2, 4 * n, units), jnp.bfloat16),
            pltpu.VMEM((4 * n, units), jnp.float32),
            pltpu.VMEM((6, units, dim), jnp.bfloat16),
            pltpu.SemaphoreType.DMA((6,)),
        ],
        compiler_params=pltpu.CompilerParams(vmem_limit_bytes=44 * 1024 * 1024),
        cost_estimate=pl.CostEstimate(
            flops=2 * 4 * n * dim * units * 6, bytes_accessed=30 << 20, transcendentals=0
        ),
    )(where, *held, *weights)


def hold_kernel(src_ref, dst_ref, sem):
    copy = pltpu.make_async_copy(src_ref, dst_ref, sem)
    copy.start()
    copy.wait()


def hold(weight):
    return pl.pallas_call(
        hold_kernel,
        out_shape=pltpu.VMEM(weight.shape, weight.dtype),
        in_specs=[pl.BlockSpec(memory_space=pltpu.HBM)],
        out_specs=pl.BlockSpec(memory_space=pltpu.VMEM),
        scratch_shapes=[pltpu.SemaphoreType.DMA],
        compiler_params=pltpu.CompilerParams(vmem_limit_bytes=8 * 1024 * 1024),
    )(weight)


def dispatch_kernel(ids_hbm, tokens_hbm, sent_ref, spots_ref, ids_ref, tokens_ref, sems):
    ids_copy = pltpu.make_async_copy(ids_hbm, ids_ref, sems.at[0])
    tokens_copy = pltpu.make_async_copy(tokens_hbm, tokens_ref, sems.at[1])
    ids_copy.start()
    tokens_copy.start()
    tok_rows, feat = tokens_ref.shape
    blocks = feat // LANES
    share = CAP // CHUNKS
    n = share // 2
    unit = blocks * n
    expert = lax.broadcasted_iota(jnp.int32, (EXPERTS, tok_rows), 0)
    ids_copy.wait()
    named = [ids_ref[k:k + 1] == expert for k in range(2)]
    chosen = (named[0] | named[1]).astype(jnp.float32).astype(jnp.bfloat16)
    before = lax.broadcasted_iota(jnp.int32, (tok_rows, tok_rows), 0)
    before = before < lax.broadcasted_iota(jnp.int32, (tok_rows, tok_rows), 1)
    before = before.astype(jnp.float32).astype(jnp.bfloat16)
    rank = jnp.dot(chosen, before, preferred_element_type=jnp.float32).astype(jnp.int32)
    chunk = (rank >= share).astype(jnp.int32)
    left = rank - chunk * share
    core = (left >= n).astype(jnp.int32)
    group = expert * 2 + core
    row = left - core * n
    spot = group * (CHUNKS * unit) + chunk * unit + row
    at = []
    for k in range(2):
        at.append(jnp.sum(jnp.where(named[k], spot, 0), axis=0, keepdims=True))
        spots_ref[k:k + 1] = at[k]
    at = [jnp.concatenate([a + l * n for l in range(blocks)], axis=1) for a in at]
    sites = sent_ref.shape[0]
    site = lax.broadcasted_iota(jnp.int32, (sites, blocks * tok_rows), 0)
    picker = ((at[0] == site) | (at[1] == site)).astype(jnp.float32).astype(jnp.bfloat16)
    tokens_copy.wait()
    tokens = jnp.concatenate(
        [tokens_ref[:, l * LANES:(l + 1) * LANES] for l in range(blocks)], axis=0
    )
    sent_ref[...] = jnp.dot(picker, tokens, preferred_element_type=jnp.float32).astype(jnp.bfloat16)


def dispatch(ids, tokens):
    tok_rows, feat = tokens.shape
    vmem = pl.BlockSpec(memory_space=pltpu.VMEM)
    return pl.pallas_call(
        dispatch_kernel,
        out_shape=[
            jax.ShapeDtypeStruct((EXPERTS * CAP * feat // LANES, LANES), jnp.bfloat16),
            jax.ShapeDtypeStruct((2, tok_rows), jnp.int32),
        ],
        in_specs=[pl.BlockSpec(memory_space=pltpu.HBM)] * 2,
        out_specs=[vmem] * 2,
        scratch_shapes=[
            pltpu.VMEM(ids.shape, ids.dtype),
            pltpu.VMEM(tokens.shape, tokens.dtype),
            pltpu.SemaphoreType.DMA((2,)),
        ],
        compiler_params=pltpu.CompilerParams(vmem_limit_bytes=64 * 1024 * 1024 - 65536),
    )(ids, tokens)


def plan_kernel(spots_ref, take_ref):
    n = CAP // CHUNKS // 2
    tok_rows = spots_ref.shape[0]
    site = lax.broadcasted_iota(jnp.int32, (tok_rows, take_ref.shape[2]), 1)
    for k in range(2):
        for l in range(take_ref.shape[0]):
            take = spots_ref[:, k:k + 1] + l * n == site
            take_ref[l, k * tok_rows:(k + 1) * tok_rows] = (
                take.astype(jnp.float32).astype(jnp.bfloat16)
            )


def combine_kernel(back_ref, take_ref, scores_ref, mixed_ref):
    tok_rows = mixed_ref.shape[0]
    for l in range(mixed_ref.shape[1] // LANES):
        mine = jnp.dot(take_ref[l], back_ref[...], preferred_element_type=jnp.float32)
        total = scores_ref[:, :1] * mine[:tok_rows] + scores_ref[:, 1:] * mine[tok_rows:]
        mixed_ref[:, l * LANES:(l + 1) * LANES] = total.astype(mixed_ref.dtype)


def local_call(kernel, out, *args):
    vmem = pl.BlockSpec(memory_space=pltpu.VMEM)
    return pl.pallas_call(
        kernel,
        out_shape=out,
        in_specs=[vmem] * len(args),
        out_specs=vmem,
        compiler_params=pltpu.CompilerParams(vmem_limit_bytes=16 * 1024 * 1024),
    )(*args)


def exchange(v):
    return lax.all_to_all(v, ("z", "c"), split_axis=0, concat_axis=0, tiled=True)


def add_up(values):
    total = values[0].astype(jnp.float32)
    for v in values[1:]:
        total = total + v.astype(jnp.float32)
    return total.astype(jnp.bfloat16)


def body(tokens, expert_ids, gate_scores, gate_weight, up_weight, down_weight):
    n_z = lax.axis_size("z")
    tok_rows, feat = tokens.shape
    core = lax.axis_index("c")
    where = jnp.stack([core, lax.axis_index("y")]).astype(jnp.int32)

    swap = [(0, 1), (1, 0)]
    weights = []
    for w in (gate_weight[0], up_weight[0], down_weight[0]):
        weights += [w, lax.ppermute(w, "c", swap)]

    n = CAP // CHUNKS // 2
    blocks = feat // LANES
    unit = blocks * n
    sent, spots = dispatch(expert_ids.T, tokens)
    spots = spots.T

    def select(matrix, v, contract):
        return lax.dot_general(
            matrix, v, (((contract,), (0,)), ((), ())), preferred_element_type=jnp.float32
        )

    size = n_z * 2 * unit
    sites = jnp.arange(size, dtype=jnp.int32)
    z_of, rest = lax.div(sites, 2 * unit), lax.rem(sites, 2 * unit)
    moved = lax.div(rest, n) * (n_z * n) + z_of * n + lax.rem(rest, n)
    shuffle = (moved[None, :] == sites[:, None]).astype(jnp.bfloat16)

    got = exchange(sent.reshape(n_z * 2, CHUNKS * unit, LANES))
    got = got.reshape(n_z * 2, CHUNKS, unit, LANES)
    here = jnp.stack([
        select(shuffle, got[:, i].reshape(size, LANES), 1).astype(jnp.bfloat16)
        for i in range(CHUNKS)
    ])

    def permute(v, axis, shift):
        return lax.ppermute(v, PLANE, ring(axis, shift))

    order = (1, 3, 2)
    near = {s: permute(here, 0, s) for s in order}
    held = []
    for i in range(CHUNKS):
        first = jnp.stack([here[i]] + [near[s][i] for s in (1, 2, 3)])
        far = {}
        for s in order:
            far[s] = permute(first, 1, s)
        held.append((first, far[1], far[2], far[3]))
    weights[0] = hold(weights[0])
    parts = [expert_part(where, h, weights) for h in held]

    backs = []
    for part in parts:
        got = [permute(part[s], 1, -s) for s in order]
        total = add_up([part[0]] + got)
        got = [permute(total[s], 0, -s) for s in order]
        back = select(shuffle, add_up([total[0]] + got), 0).astype(jnp.bfloat16)
        backs.append(back.reshape(n_z * 2, unit, LANES))

    back = exchange(jnp.concatenate(backs, axis=1)).reshape(CHUNKS * size, LANES)
    tok_rows = tokens.shape[0]
    take = local_call(
        plan_kernel,
        jax.ShapeDtypeStruct((blocks, 2 * tok_rows, CHUNKS * size), jnp.bfloat16),
        spots,
    )
    return local_call(
        combine_kernel, jax.ShapeDtypeStruct(tokens.shape, tokens.dtype), back, take, gate_scores
    )


def solution(mesh):
    n_ep = mesh.shape["ep"]
    fine = Mesh(mesh.devices.reshape(n_ep // NX, NX, NY, 2), ("z", "x", "y", "c"))
    ep, fsdp = ("z", "x"), ("y", "c")
    in_specs = (
        P(ep, fsdp),
        P(ep, None),
        P(ep, None),
        P(ep, fsdp, None),
        P(ep, fsdp, None),
        P(ep, fsdp, None),
    )

    return jax.shard_map(body, mesh=fine, in_specs=in_specs, out_specs=P(ep, fsdp), check_vma=False)
```
